128 devices in a mesh: layer: 4 (over z_hi, core), grid: 32 (over y, x, z_lo).
Axes of the slice: x: 4, y: 4, z: 4 (z_hi: 2, z_lo: 2; z = z_hi * 2 + z_lo), core: 2. Of those that a mesh axis runs over, the one named last changes fastest.
Arguments:
- fourier: float32 [1024, 512, 256], P(('layer', 'grid')), may hold values from -6 to 6
- weights: float32 [1024], P(('layer', 'grid')), may hold values from 0.009375 to 0.09375
- legendre: float32 [256, 513, 1024], P('grid'), may hold values from -6 to 6
- pair_slots: int32 [256], replicated, may hold values from 0 to 255, each once
Outputs:
- spectra: float32 [256, 513, 256], P('grid', None, 'layer')
The draws below stay inside these ranges and needn't reach their ends.
Inputs may be any that keep to these rules, and one draw needn't show every extreme that they name: Each pair index appears exactly once; position q holds wavenumbers pair_slots[q] and 511 - pair_slots[q].
All inputs are finite; a program needn't handle non-finite values.
Results may differ from the reference program's by a relative error of at most 0.0003.
Values sent between devices are 32-bit elements; how exact they have to be, the bound alone decides.
No kernel may reach another device: no remote copies, remote signals or barrier semaphores. Data moves between devices by JAX's collectives and lax.ppermute only.
A program may use at most 128 MiB of HBM per device.

```python
import math
import jax
import jax.numpy as jnp
from jax import lax

M = 512
J = 1024
C = 256
PAIRS = 256


def steps_of(rng, extent, shards, low, top_value):
    gain, own = 1.0, jax.random.fold_in(rng, 6)
    for position, shards_of in shards:
        steps = jnp.exp(jax.random.uniform(jax.random.fold_in(own, position), (shards_of,), jnp.float32, low / len(shards), top_value / len(shards)))
        gain = gain * jnp.repeat(steps, extent[position] // shards_of).reshape([-1 if axis == position else 1 for axis in range(len(extent))])
    return gain


def normal_values(own_key, extent, scale, reach, cuts=(), kind=jnp.bfloat16):
    values = scale * jax.random.normal(own_key, extent, jnp.float32)
    if cuts:
        values = values * steps_of(own_key, extent, cuts, -0.22, 0.18)
    return jnp.clip(values, -reach, reach).astype(kind)


def setup_inputs(seed: int = 0) -> dict:
    keys = jax.random.split(jax.random.key(seed), 5)
    fourier = normal_values(keys[0], (J, M, C), 1.0, 6.0, ((0, 128),), jnp.float32)
    weights = jnp.clip(jnp.exp(math.log(0.09375) - 2.3025851 * jax.random.uniform(keys[1], (J,), jnp.float32) ** steps_of(keys[1], (J,), ((0, 128),), -0.2, 0.2)), 0.009375, 0.09375)
    legendre = normal_values(keys[2], (PAIRS, M + 1, J), 1.0, 6.0, ((0, 32),), jnp.float32)
    pair_slots = jax.random.permutation(keys[3], PAIRS).astype(jnp.int32)
    return dict(fourier=fourier, weights=weights, legendre=legendre, pair_slots=pair_slots)


def reference(fourier, weights, legendre, pair_slots):
    scaled = fourier * weights[:, None, None]
    row_ids = jnp.arange(M + 1, dtype=jnp.int32)
    fields_count = scaled.shape[2]

    def pair_block(inputs):
        poly_block, slot_value = inputs
        wave_first = slot_value.astype(jnp.int32)
        wave_second = (M - 1 - slot_value).astype(jnp.int32)
        first_values = lax.dynamic_index_in_dim(scaled, wave_first, 1, keepdims=False)
        second_values = lax.dynamic_index_in_dim(scaled, wave_second, 1, keepdims=False)
        stacked = jnp.concatenate([first_values, second_values], axis=1)
        product = jnp.dot(poly_block, stacked, precision=lax.Precision.HIGHEST, preferred_element_type=jnp.float32)
        in_first = row_ids[:, None] < (M - wave_first)
        return jnp.where(in_first, product[:, :fields_count], product[:, fields_count:])

    return lax.map(pair_block, (legendre, pair_slots))
```

```python
import functools

import jax
import jax.numpy as jnp
import numpy as np
from jax import lax
from jax.experimental import pallas as pl
from jax.experimental.pallas import tpu as pltpu
from jax.sharding import Mesh, PartitionSpec as P

AXES = ("zh", "core", "y", "x", "zl")
SIZES = (2, 2, 4, 4, 2)
LAYER = ("zh", "core")
GRID = ("y", "x", "zl")
ORDER = ("zh", "zl", "x", "y", "core")

LATS = 8
PAIRS = 8
LANES = 128
HALF = 64
PITCH = 520
ROWS = 528
VMEM = 60 * 2**20
STEP = 176


def exchange_places():
    ids = np.arange(np.prod(SIZES)).reshape(SIZES)
    order = ids.transpose([AXES.index(a) for a in ORDER]).reshape(-1)
    place = np.empty_like(order)
    place[order] = np.arange(order.size)
    return place


PLACE = exchange_places()


def pack_kernel(slots, weights, fourier, out, rows, blocks, sems, sent):
    waves = fourier.shape[1]

    def fetch(half, lat):
        return pltpu.make_async_copy(
            fourier.at[lat, :, pl.ds(half * LANES, LANES)],
            rows.at[half, pl.ds(lat * PITCH, waves), :],
            sems.at[half, lat],
        )

    for half in range(2):
        for lat in range(LATS):
            fetch(half, lat).start()
    lat_ids = lax.broadcasted_iota(jnp.int32, (LATS, LANES), 0)
    scale = jnp.zeros((LATS, LANES), jnp.float32)
    for lat in range(LATS):
        scale = jnp.where(lat_ids == lat, weights[lat], scale)
    low = lax.broadcasted_iota(jnp.int32, (LATS, LANES), 1) < HALF
    for half in range(2):
        for lat in range(LATS):
            fetch(half, lat).wait()

        @pl.loop(0, 32)
        def _(i):
            zl, x, y = i // 16, (i // 4) % 4, i % 4
            g = (y * 4 + x) * 2 + zl
            place = (half * 32 + i) * 2
            for q in range(PAIRS):
                first = slots[g * PAIRS + q]
                second = waves - 1 - first
                a = rows[half, pl.ds(first, LATS, stride=PITCH), :] * scale
                b = rows[half, pl.ds(second, LATS, stride=PITCH), :] * scale
                turned = pltpu.roll(b, HALF, 1)
                blocks[place, q] = jnp.where(low, a, turned)
                blocks[place + 1, q] = jnp.where(low, turned, a)
            pltpu.make_async_copy(blocks.at[pl.ds(place, 2)], out.at[pl.ds(place, 2)], sent).start()

    pltpu.make_async_copy(blocks, out, sent).wait()


def pack(pair_slots, weights, fourier):
    devices = int(np.prod(SIZES))
    return pl.pallas_call(
        pack_kernel,
        name="pack",
        out_shape=jax.ShapeDtypeStruct((devices, PAIRS, LATS, LANES), jnp.float32),
        in_specs=[
            pl.BlockSpec(memory_space=pltpu.SMEM),
            pl.BlockSpec(memory_space=pltpu.SMEM),
            pl.BlockSpec(memory_space=pl.ANY),
        ],
        out_specs=pl.BlockSpec(memory_space=pl.ANY),
        scratch_shapes=[
            pltpu.VMEM((2, LATS * PITCH, LANES), jnp.float32),
            pltpu.VMEM((devices, PAIRS, LATS, LANES), jnp.float32),
            pltpu.SemaphoreType.DMA((2, LATS)),
            pltpu.SemaphoreType.DMA,
        ],
        compiler_params=pltpu.CompilerParams(vmem_limit_bytes=VMEM),
        cost_estimate=pl.CostEstimate(flops=4 * 2**20, bytes_accessed=8 * 2**20, transcendentals=0),
    )(pair_slots, weights, fourier)


def split_kernel(legendre, high, low):
    rows = legendre.shape[0] // PAIRS
    for q in range(PAIRS):
        part = legendre[pl.ds(q, rows, stride=PAIRS), :]
        top = part.astype(jnp.bfloat16)
        high[q] = top
        low[q] = (part - top.astype(jnp.float32)).astype(jnp.bfloat16)


def split(legendre):
    lats = legendre.shape[1]
    shape = jax.ShapeDtypeStruct((PAIRS, ROWS, lats), jnp.bfloat16)
    spec = pl.BlockSpec((PAIRS, STEP, LANES), lambda i, j: (0, i, j))
    return pl.pallas_call(
        split_kernel,
        name="split",
        grid=(ROWS // STEP, lats // LANES),
        out_shape=(shape, shape),
        in_specs=[pl.BlockSpec((STEP * PAIRS, LANES), lambda i, j: (i, j))],
        out_specs=(spec, spec),
        compiler_params=pltpu.CompilerParams(vmem_limit_bytes=VMEM),
        cost_estimate=pl.CostEstimate(flops=2 * 10**10, bytes_accessed=32 * 2**20, transcendentals=0),
    )(legendre)


def sum_kernel(slots, where, high, low, values, out, terms):
    degrees = out.shape[2]
    q = pl.program_id(0)
    for d in range(0, len(PLACE), 2):
        value = jnp.concatenate([values[int(PLACE[d]), 0], values[int(PLACE[d + 1]), 0]], axis=0)
        top = value.astype(jnp.bfloat16)
        terms[d * LATS : (d + 2) * LATS, :LANES] = top
        terms[d * LATS : (d + 2) * LATS, LANES:] = (value - top.astype(jnp.float32)).astype(jnp.bfloat16)
    dot = functools.partial(jnp.dot, preferred_element_type=jnp.float32)
    wide = dot(high[0], terms[...])
    total = wide[:, :LANES] + wide[:, LANES:] + dot(low[0], terms[:, :LANES])
    turned = total.T[:, :degrees]
    limit = degrees - 1 - slots[where[0] * PAIRS + q]
    in_first = lax.broadcasted_iota(jnp.int32, (HALF, degrees), 1) < limit
    in_low = jnp.logical_xor(in_first, where[1] == 1)
    out[0] = jnp.where(in_low, turned[:HALF], turned[HALF:])


def sums(pair_slots, where, high, low, values, degrees):
    lats = high.shape[2]
    matrix = pl.BlockSpec((1, ROWS, lats), lambda q: (q, 0, 0))
    return pl.pallas_call(
        sum_kernel,
        name="sums",
        grid=(PAIRS,),
        out_shape=jax.ShapeDtypeStruct((PAIRS, HALF, degrees), jnp.float32),
        in_specs=[
            pl.BlockSpec(memory_space=pltpu.SMEM),
            pl.BlockSpec(memory_space=pltpu.SMEM),
            matrix,
            matrix,
            pl.BlockSpec((values.shape[0], 1, LATS, LANES), lambda q: (0, q, 0, 0)),
        ],
        out_specs=pl.BlockSpec((1, HALF, degrees), lambda q: (q, 0, 0)),
        scratch_shapes=[pltpu.VMEM((lats, 2 * LANES), jnp.bfloat16)],
        compiler_params=pltpu.CompilerParams(vmem_limit_bytes=VMEM),
        cost_estimate=pl.CostEstimate(flops=6 * 2**30, bytes_accessed=24 * 2**20, transcendentals=0),
    )(pair_slots, where, high, low, values)


def shards(fourier, weights, legendre, pair_slots):
    degrees, lats = legendre.shape[1:]
    packed = pack(pair_slots, weights, fourier)
    owned = lax.all_to_all(packed, ORDER, split_axis=0, concat_axis=0, tiled=True)
    high, low = split(jnp.transpose(legendre, (1, 0, 2)).reshape(degrees * PAIRS, lats))
    where = jnp.stack([lax.axis_index(GRID), lax.axis_index("core")]).astype(jnp.int32)
    result = sums(pair_slots, where, high, low, owned, degrees)
    return jnp.transpose(result, (0, 2, 1))


def solution(mesh):
    parts = Mesh(mesh.devices.reshape(SIZES), AXES)
    in_specs = (P(AXES, None, None), P(AXES), P(GRID, None, None), P())
    out_specs = P(GRID, None, LAYER)
    return jax.shard_map(shards, mesh=parts, in_specs=in_specs, out_specs=out_specs, check_vma=False)
```

```python
import functools

import jax
import jax.numpy as jnp
import numpy as np
from jax import lax
from jax.experimental import pallas as pl
from jax.experimental.pallas import tpu as pltpu
from jax.sharding import Mesh, PartitionSpec as P

AXES = ("zh", "core", "y", "x", "zl")
SIZES = (2, 2, 4, 4, 2)
LAYER = ("zh", "core")
GRID = ("y", "x", "zl")
ORDER = ("zh", "zl", "x", "y", "core")

LATS = 8
PAIRS = 8
LANES = 128
HALF = 64
PITCH = 520
ROWS = 528
HELD = 3
DEPTH = 3
PARTS = 1
UNROLL = 2
VMEM = 60 * 2**20
STEP = 176


def exchange_places():
    ids = np.arange(np.prod(SIZES)).reshape(SIZES)
    order = ids.transpose([AXES.index(a) for a in ORDER]).reshape(-1)
    place = np.empty_like(order)
    place[order] = np.arange(order.size)
    return place


PLACE = exchange_places()


def pack_kernel(part, slots_in, weights_in, fourier, out, slots, weights, rows, blocks, sems, sent, small):
    waves = fourier.shape[1]
    pairs = blocks.shape[1]
    tables = (
        pltpu.make_async_copy(slots_in, slots, small.at[0]),
        pltpu.make_async_copy(weights_in, weights, small.at[1]),
    )
    for copy in tables:
        copy.start()

    def fetch(half, lat):
        return pltpu.make_async_copy(
            fourier.at[lat, :, pl.ds(half * LANES, LANES)],
            rows.at[half, pl.ds(lat * PITCH, waves), :],
            sems.at[half, lat],
        )

    for half in range(2):
        for lat in range(LATS):
            fetch(half, lat).start()
    for copy in tables:
        copy.wait()
    lat_ids = lax.broadcasted_iota(jnp.int32, (LATS, LANES), 0)
    scale = jnp.zeros((LATS, LANES), jnp.float32)
    for lat in range(LATS):
        scale = jnp.where(lat_ids == lat, weights[lat], scale)
    low = lax.broadcasted_iota(jnp.int32, (LATS, LANES), 1) < HALF
    for half in range(2):
        for lat in range(LATS):
            fetch(half, lat).wait()

        @pl.loop(0, 8 // UNROLL)
        def _(turn):
            for u in range(UNROLL):
                step = turn * UNROLL + u
                zl, x = step >> 2, step & 3
                for y in range(4):
                    place = half * 64 + step * 8 + y * 2
                    for q in range(pairs):
                        first = slots[(x * 2 + zl) * PAIRS + (y * 8 * PAIRS + part * pairs + q)]
                        second = waves - 1 - first
                        a = rows[half, pl.ds(first, LATS, stride=PITCH), :] * scale
                        b = rows[half, pl.ds(second, LATS, stride=PITCH), :] * scale
                        turned = pltpu.roll(b, HALF, 1)
                        blocks[place, q] = jnp.where(low, a, turned)
                        blocks[place + 1, q] = jnp.where(low, turned, a)
            at = pl.ds(half * 64 + turn * UNROLL * 8, UNROLL * 8)
            pltpu.make_async_copy(blocks.at[at], out.at[at], sent).start()

    pltpu.make_async_copy(blocks, out, sent).wait()


def pack(part, pair_slots, weights, fourier):
    shape = (int(np.prod(SIZES)), PAIRS // PARTS, LATS, LANES)
    return pl.pallas_call(
        functools.partial(pack_kernel, part),
        name="pack",
        out_shape=jax.ShapeDtypeStruct(shape, jnp.float32),
        in_specs=[pl.BlockSpec(memory_space=pl.ANY)] * 3,
        out_specs=pl.BlockSpec(memory_space=pl.ANY),
        scratch_shapes=[
            pltpu.SMEM(pair_slots.shape, jnp.int32),
            pltpu.SMEM(weights.shape, jnp.float32),
            pltpu.VMEM((2, LATS * PITCH, LANES), jnp.float32),
            pltpu.VMEM(shape, jnp.float32),
            pltpu.SemaphoreType.DMA((2, LATS)),
            pltpu.SemaphoreType.DMA,
            pltpu.SemaphoreType.DMA((2,)),
        ],
        compiler_params=pltpu.CompilerParams(vmem_limit_bytes=VMEM),
        cost_estimate=pl.CostEstimate(flops=4 * 2**20, bytes_accessed=8 * 2**20, transcendentals=0),
    )(pair_slots, weights, fourier)


def split_kernel(legendre, high, low):
    rows = legendre.shape[0] // PAIRS
    for q in range(PAIRS):
        part = legendre[pl.ds(q, rows, stride=PAIRS), :]
        top = part.astype(jnp.bfloat16)
        high[q] = top
        low[q] = (part - top.astype(jnp.float32)).astype(jnp.bfloat16)


def split(legendre):
    lats = legendre.shape[1]
    shape = jax.ShapeDtypeStruct((PAIRS, ROWS, lats), jnp.bfloat16)
    spec = pl.BlockSpec((PAIRS, STEP, LANES), lambda i, j: (0, i, j))
    return pl.pallas_call(
        split_kernel,
        name="split",
        grid=(ROWS // STEP, lats // LANES),
        out_shape=(shape, shape),
        in_specs=[pl.BlockSpec((STEP * PAIRS, LANES), lambda i, j: (i, j))],
        out_specs=(spec, spec),
        compiler_params=pltpu.CompilerParams(vmem_limit_bytes=VMEM),
        cost_estimate=pl.CostEstimate(flops=2 * 10**10, bytes_accessed=32 * 2**20, transcendentals=0),
    )(legendre)


def hold_kernel(high, low, *rest):
    outs, sems = rest[:-1], rest[-1]
    copies = []
    for i, out in enumerate(outs):
        source = (high, low)[i % 2].at[i // 2]
        copies.append(pltpu.make_async_copy(source, out, sems.at[i]))
    for copy in copies:
        copy.start()
    for copy in copies:
        copy.wait()


def hold(high, low):
    shape = pltpu.VMEM(high.shape[1:], high.dtype)
    return pl.pallas_call(
        hold_kernel,
        name="hold",
        out_shape=[shape] * HELD,
        in_specs=[pl.BlockSpec(memory_space=pl.ANY)] * 2,
        out_specs=[pl.BlockSpec(memory_space=pltpu.VMEM)] * HELD,
        scratch_shapes=[pltpu.SemaphoreType.DMA((HELD,))],
        compiler_params=pltpu.CompilerParams(vmem_limit_bytes=20 * 2**20),
        cost_estimate=pl.CostEstimate(flops=2 * 10**9, bytes_accessed=4 * 2**20, transcendentals=0),
    )(high, low)


def sum_kernel(part, slots_in, where_in, high, low, values, *rest):
    held, out, scratch = rest[:HELD], rest[HELD], rest[HELD + 1 :]
    slots, where, highs, lows, inputs, results, terms, sums, sems, sent, small = scratch
    pairs, _, degrees = results.shape
    tables = (
        pltpu.make_async_copy(slots_in, slots, small.at[0]),
        pltpu.make_async_copy(where_in, where, small.at[1]),
    )

    def fetch_values(q):
        return pltpu.make_async_copy(values.at[:, q], inputs.at[q], sems.at[0, q])

    def fetch_matrix(q):
        terms_of = ((high, highs), (low, lows))
        return [
            pltpu.make_async_copy(source.at[part * pairs + q], target.at[q % DEPTH], sems.at[1 + i, q])
            for i, (source, target) in enumerate(terms_of)
            if 2 * q + i >= HELD
        ]

    def matrix(q, low_term):
        at = 2 * q + low_term
        return held[at][...] if at < HELD else (highs, lows)[low_term][q % DEPTH]

    def start(q):
        if q < pairs:
            for copy in fetch_matrix(q):
                copy.start()
        if q + 1 < pairs:
            fetch_values(q + 1).start()

    def prepare(q):
        for d in range(0, len(PLACE), 2):
            value = jnp.concatenate([inputs[q, int(PLACE[d])], inputs[q, int(PLACE[d + 1])]], axis=0)
            top = value.astype(jnp.bfloat16)
            at = pl.ds(d * LATS, 2 * LATS)
            terms[q % 2, at, :LANES] = top
            terms[q % 2, at, LANES:] = (value - top.astype(jnp.float32)).astype(jnp.bfloat16)

    def multiply(q):
        dot = functools.partial(jnp.dot, preferred_element_type=jnp.float32)
        wide = dot(matrix(q, 0), terms[q % 2])
        sums[q % 2] = wide[:, :LANES] + wide[:, LANES:] + dot(matrix(q, 1), terms[q % 2, :, :LANES])

    def finish(q):
        turned = sums[q % 2].T[:, :degrees]
        limit = degrees - 1 - slots[where[0] * PAIRS + part * pairs + q]
        in_first = lax.broadcasted_iota(jnp.int32, (HALF, degrees), 1) < limit
        in_low = jnp.logical_xor(in_first, where[1] == 1)
        results[q] = jnp.where(in_low, turned[:HALF], turned[HALF:])

    def send(q):
        pltpu.make_async_copy(results.at[q], out.at[q], sent).start()

    fetch_values(0).start()
    for q in range(DEPTH - 1):
        start(q)
    for copy in tables:
        copy.start()
    for copy in tables:
        copy.wait()
    fetch_values(0).wait()
    prepare(0)
    for q in range(pairs):
        start(q + DEPTH - 1)
        for copy in fetch_matrix(q):
            copy.wait()
        if q + 1 < pairs:
            fetch_values(q + 1).wait()
            prepare(q + 1)
        multiply(q)
        if q:
            finish(q - 1)
            send(q - 1)
    finish(pairs - 1)
    send(pairs - 1)
    pltpu.make_async_copy(results, out, sent).wait()


def sums(part, pair_slots, where, high, low, values, held, degrees):
    lats = high.shape[2]
    devices, pairs = values.shape[:2]
    any_space = pl.BlockSpec(memory_space=pl.ANY)
    return pl.pallas_call(
        functools.partial(sum_kernel, part),
        name="sums",
        out_shape=jax.ShapeDtypeStruct((pairs, HALF, degrees), jnp.float32),
        in_specs=[any_space] * 5 + [pl.BlockSpec(memory_space=pltpu.VMEM)] * HELD,
        out_specs=any_space,
        scratch_shapes=[
            pltpu.SMEM(pair_slots.shape, jnp.int32),
            pltpu.SMEM(where.shape, jnp.int32),
            pltpu.VMEM((DEPTH, ROWS, lats), jnp.bfloat16),
            pltpu.VMEM((DEPTH, ROWS, lats), jnp.bfloat16),
            pltpu.VMEM((pairs, devices, LATS, LANES), jnp.float32),
            pltpu.VMEM((pairs, HALF, degrees), jnp.float32),
            pltpu.VMEM((2, lats, 2 * LANES), jnp.bfloat16),
            pltpu.VMEM((2, ROWS, LANES), jnp.float32),
            pltpu.SemaphoreType.DMA((3, pairs)),
            pltpu.SemaphoreType.DMA,
            pltpu.SemaphoreType.DMA((2,)),
        ],
        compiler_params=pltpu.CompilerParams(vmem_limit_bytes=40 * 2**20),
        cost_estimate=pl.CostEstimate(flops=6 * 2**30 // PARTS, bytes_accessed=24 * 2**20 // PARTS, transcendentals=0),
    )(pair_slots, where, high, low, values, *held)


def shards(fourier, weights, legendre, pair_slots):
    degrees, lats = legendre.shape[1:]
    owned = []
    for part in range(PARTS):
        packed = pack(part, pair_slots, weights, fourier)
        owned.append(lax.all_to_all(packed, ORDER, split_axis=0, concat_axis=0, tiled=True))
    high, low = split(jnp.transpose(legendre, (1, 0, 2)).reshape(degrees * PAIRS, lats))
    held = hold(high, low)
    where = jnp.stack([lax.axis_index(GRID), lax.axis_index("core")]).astype(jnp.int32)
    results = [sums(part, pair_slots, where, high, low, owned[part], held, degrees) for part in range(PARTS)]
    result = results[0] if PARTS == 1 else jnp.concatenate(results, axis=0)
    return jnp.transpose(result, (0, 2, 1))


def solution(mesh):
    parts = Mesh(mesh.devices.reshape(SIZES), AXES)
    in_specs = (P(AXES, None, None), P(AXES), P(GRID, None, None), P())
    out_specs = P(GRID, None, LAYER)
    return jax.shard_map(shards, mesh=parts, in_specs=in_specs, out_specs=out_specs, check_vma=False)
```

```python
import functools

import jax
import jax.numpy as jnp
import numpy as np
from jax import lax
from jax.experimental import pallas as pl
from jax.experimental.pallas import tpu as pltpu
from jax.sharding import Mesh, PartitionSpec as P

AXES = ("zh", "core", "y", "x", "zl")
SIZES = (2, 2, 4, 4, 2)
LAYER = ("zh", "core")
GRID = ("y", "x", "zl")
ORDER = ("zh", "zl", "x", "y", "core")

LATS = 8
PAIRS = 8
LANES = 128
HALF = 64
PITCH = 520
ROWS = 528
HELD = 3
DEPTH = 4
PARTS = 1
UNROLL = 2
VMEM = 60 * 2**20
STEP = 176


def exchange_places():
    ids = np.arange(np.prod(SIZES)).reshape(SIZES)
    order = ids.transpose([AXES.index(a) for a in ORDER]).reshape(-1)
    place = np.empty_like(order)
    place[order] = np.arange(order.size)
    return place


PLACE = exchange_places()


def pack_kernel(part, slots_in, weights_in, fourier, out, slots, weights, rows, blocks, sems, sent, small):
    waves = fourier.shape[1]
    pairs = blocks.shape[1]
    tables = (
        pltpu.make_async_copy(slots_in, slots, small.at[0]),
        pltpu.make_async_copy(weights_in, weights, small.at[1]),
    )
    for copy in tables:
        copy.start()

    def fetch(half, lat):
        return pltpu.make_async_copy(
            fourier.at[lat, :, pl.ds(half * LANES, LANES)],
            rows.at[half, pl.ds(lat * PITCH, waves), :],
            sems.at[half, lat],
        )

    for half in range(2):
        for lat in range(LATS):
            fetch(half, lat).start()
    for copy in tables:
        copy.wait()
    lat_ids = lax.broadcasted_iota(jnp.int32, (LATS, LANES), 0)
    scale = jnp.zeros((LATS, LANES), jnp.float32)
    for lat in range(LATS):
        scale = jnp.where(lat_ids == lat, weights[lat], scale)
    low = lax.broadcasted_iota(jnp.int32, (LATS, LANES), 1) < HALF
    for half in range(2):
        for lat in range(LATS):
            fetch(half, lat).wait()

        @pl.loop(0, 8 // UNROLL)
        def _(turn):
            for u in range(UNROLL):
                step = turn * UNROLL + u
                zl, x = step >> 2, step & 3
                for y in range(4):
                    place = half * 64 + step * 8 + y * 2
                    for q in range(pairs):
                        first = slots[(x * 2 + zl) * PAIRS + (y * 8 * PAIRS + part * pairs + q)]
                        second = waves - 1 - first
                        a = rows[half, pl.ds(first, LATS, stride=PITCH), :] * scale
                        b = rows[half, pl.ds(second, LATS, stride=PITCH), :] * scale
                        turned = pltpu.roll(b, HALF, 1)
                        blocks[place, q] = jnp.where(low, a, turned)
                        blocks[place + 1, q] = jnp.where(low, turned, a)
            at = pl.ds(half * 64 + turn * UNROLL * 8, UNROLL * 8)
            pltpu.make_async_copy(blocks.at[at], out.at[at], sent).start()

    pltpu.make_async_copy(blocks, out, sent).wait()


def pack(part, pair_slots, weights, fourier):
    shape = (int(np.prod(SIZES)), PAIRS // PARTS, LATS, LANES)
    return pl.pallas_call(
        functools.partial(pack_kernel, part),
        name="pack",
        out_shape=jax.ShapeDtypeStruct(shape, jnp.float32),
        in_specs=[pl.BlockSpec(memory_space=pl.ANY)] * 3,
        out_specs=pl.BlockSpec(memory_space=pl.ANY),
        scratch_shapes=[
            pltpu.SMEM(pair_slots.shape, jnp.int32),
            pltpu.SMEM(weights.shape, jnp.float32),
            pltpu.VMEM((2, LATS * PITCH, LANES), jnp.float32),
            pltpu.VMEM(shape, jnp.float32),
            pltpu.SemaphoreType.DMA((2, LATS)),
            pltpu.SemaphoreType.DMA,
            pltpu.SemaphoreType.DMA((2,)),
        ],
        compiler_params=pltpu.CompilerParams(vmem_limit_bytes=VMEM),
        cost_estimate=pl.CostEstimate(flops=4 * 2**20, bytes_accessed=8 * 2**20, transcendentals=0),
    )(pair_slots, weights, fourier)


def split_kernel(legendre, high, low):
    rows = legendre.shape[0] // PAIRS
    for q in range(PAIRS):
        part = legendre[pl.ds(q, rows, stride=PAIRS), :]
        top = part.astype(jnp.bfloat16)
        high[q] = top
        low[q] = (part - top.astype(jnp.float32)).astype(jnp.bfloat16)


def split(legendre):
    lats = legendre.shape[1]
    shape = jax.ShapeDtypeStruct((PAIRS, ROWS, lats), jnp.bfloat16)
    spec = pl.BlockSpec((PAIRS, STEP, LANES), lambda i, j: (0, i, j))
    return pl.pallas_call(
        split_kernel,
        name="split",
        grid=(ROWS // STEP, lats // LANES),
        out_shape=(shape, shape),
        in_specs=[pl.BlockSpec((STEP * PAIRS, LANES), lambda i, j: (i, j))],
        out_specs=(spec, spec),
        compiler_params=pltpu.CompilerParams(vmem_limit_bytes=VMEM),
        cost_estimate=pl.CostEstimate(flops=2 * 10**10, bytes_accessed=32 * 2**20, transcendentals=0),
    )(legendre)


def hold_kernel(high, low, *rest):
    outs, sems = rest[:-1], rest[-1]
    copies = []
    for i, out in enumerate(outs):
        source = (high, low)[i % 2].at[i // 2]
        copies.append(pltpu.make_async_copy(source, out, sems.at[i]))
    for copy in copies:
        copy.start()
    for copy in copies:
        copy.wait()


def hold(high, low):
    shape = pltpu.VMEM(high.shape[1:], high.dtype)
    return pl.pallas_call(
        hold_kernel,
        name="hold",
        out_shape=[shape] * HELD,
        in_specs=[pl.BlockSpec(memory_space=pl.ANY)] * 2,
        out_specs=[pl.BlockSpec(memory_space=pltpu.VMEM)] * HELD,
        scratch_shapes=[pltpu.SemaphoreType.DMA((HELD,))],
        compiler_params=pltpu.CompilerParams(vmem_limit_bytes=20 * 2**20),
        cost_estimate=pl.CostEstimate(flops=2 * 10**9, bytes_accessed=4 * 2**20, transcendentals=0),
    )(high, low)


def sum_kernel(part, slots_in, where_in, high, low, values, *rest):
    held, out, scratch = rest[:HELD], rest[HELD], rest[HELD + 1 :]
    slots, where, highs, lows, inputs, results, terms, sums, sems, sent, small = scratch
    pairs, _, degrees = results.shape
    tables = (
        pltpu.make_async_copy(slots_in, slots, small.at[0]),
        pltpu.make_async_copy(where_in, where, small.at[1]),
    )

    def fetch_values(q):
        return pltpu.make_async_copy(values.at[:, q], inputs.at[q], sems.at[0, q])

    def fetch_matrix(q):
        terms_of = ((high, highs), (low, lows))
        return [
            pltpu.make_async_copy(source.at[part * pairs + q], target.at[q % DEPTH], sems.at[1 + i, q])
            for i, (source, target) in enumerate(terms_of)
            if 2 * q + i >= HELD
        ]

    def matrix(q, low_term):
        at = 2 * q + low_term
        return held[at][...] if at < HELD else (highs, lows)[low_term][q % DEPTH]

    def start(q):
        if q < pairs:
            for copy in fetch_matrix(q):
                copy.start()
        if q + 1 < pairs:
            fetch_values(q + 1).start()

    def prepare(q):
        for d, place in enumerate(PLACE):
            value = inputs[q, int(place)]
            top = value.astype(jnp.bfloat16)
            at = pl.ds(d * LATS, LATS)
            terms[q % 2, at, :LANES] = top
            terms[q % 2, at, LANES:] = (value - top.astype(jnp.float32)).astype(jnp.bfloat16)

    def multiply(q):
        dot = functools.partial(jnp.dot, preferred_element_type=jnp.float32)
        wide = dot(matrix(q, 0), terms[q % 2])
        sums[q % 2] = wide[:, :LANES] + wide[:, LANES:] + dot(matrix(q, 1), terms[q % 2, :, :LANES])

    def finish(q):
        turned = sums[q % 2].T[:, :degrees]
        limit = degrees - 1 - slots[where[0] * PAIRS + part * pairs + q]
        in_first = lax.broadcasted_iota(jnp.int32, (HALF, degrees), 1) < limit
        in_low = jnp.logical_xor(in_first, where[1] == 1)
        results[q] = jnp.where(in_low, turned[:HALF], turned[HALF:])

    def send(q):
        pltpu.make_async_copy(results.at[q], out.at[q], sent).start()

    fetch_values(0).start()
    for q in range(DEPTH - 1):
        start(q)
    for copy in tables:
        copy.start()
    fetch_values(0).wait()
    prepare(0)
    for q in range(pairs):
        start(q + DEPTH - 1)
        for copy in fetch_matrix(q):
            copy.wait()
        if q + 1 < pairs:
            fetch_values(q + 1).wait()
            prepare(q + 1)
        if q == 1:
            for copy in tables:
                copy.wait()
        multiply(q)
        if q:
            finish(q - 1)
            send(q - 1)
    finish(pairs - 1)
    send(pairs - 1)
    pltpu.make_async_copy(results, out, sent).wait()


def sums(part, pair_slots, where, high, low, values, held, degrees):
    lats = high.shape[2]
    devices, pairs = values.shape[:2]
    any_space = pl.BlockSpec(memory_space=pl.ANY)
    return pl.pallas_call(
        functools.partial(sum_kernel, part),
        name="sums",
        out_shape=jax.ShapeDtypeStruct((pairs, HALF, degrees), jnp.float32),
        in_specs=[any_space] * 5 + [pl.BlockSpec(memory_space=pltpu.VMEM)] * HELD,
        out_specs=any_space,
        scratch_shapes=[
            pltpu.SMEM(pair_slots.shape, jnp.int32),
            pltpu.SMEM(where.shape, jnp.int32),
            pltpu.VMEM((DEPTH, ROWS, lats), jnp.bfloat16),
            pltpu.VMEM((DEPTH, ROWS, lats), jnp.bfloat16),
            pltpu.VMEM((pairs, devices, LATS, LANES), jnp.float32),
            pltpu.VMEM((pairs, HALF, degrees), jnp.float32),
            pltpu.VMEM((2, lats, 2 * LANES), jnp.bfloat16),
            pltpu.VMEM((2, ROWS, LANES), jnp.float32),
            pltpu.SemaphoreType.DMA((3, pairs)),
            pltpu.SemaphoreType.DMA,
            pltpu.SemaphoreType.DMA((2,)),
        ],
        compiler_params=pltpu.CompilerParams(
            vmem_limit_bytes=40 * 2**20,
        ),
        cost_estimate=pl.CostEstimate(flops=6 * 2**30 // PARTS, bytes_accessed=24 * 2**20 // PARTS, transcendentals=0),
    )(pair_slots, where, high, low, values, *held)


def shards(fourier, weights, legendre, pair_slots):
    degrees, lats = legendre.shape[1:]
    owned = []
    for part in range(PARTS):
        packed = pack(part, pair_slots, weights, fourier)
        owned.append(lax.all_to_all(packed, ORDER, split_axis=0, concat_axis=0, tiled=True))
    high, low = split(jnp.transpose(legendre, (1, 0, 2)).reshape(degrees * PAIRS, lats))
    held = hold(high, low)
    where = jnp.stack([lax.axis_index(GRID), lax.axis_index("core")]).astype(jnp.int32)
    results = [sums(part, pair_slots, where, high, low, owned[part], held, degrees) for part in range(PARTS)]
    result = results[0] if PARTS == 1 else jnp.concatenate(results, axis=0)
    return jnp.transpose(result, (0, 2, 1))


def solution(mesh):
    parts = Mesh(mesh.devices.reshape(SIZES), AXES)
    in_specs = (P(AXES, None, None), P(AXES), P(GRID, None, None), P())
    out_specs = P(GRID, None, LAYER)
    return jax.shard_map(shards, mesh=parts, in_specs=in_specs, out_specs=out_specs, check_vma=False)
```

```python
import functools

import jax
import jax.numpy as jnp
import numpy as np
from jax import lax
from jax.experimental import pallas as pl
from jax.experimental.pallas import tpu as pltpu
from jax.sharding import Mesh, PartitionSpec as P

AXES = ("zh", "core", "y", "x", "zl")
SIZES = (2, 2, 4, 4, 2)
LAYER = ("zh", "core")
GRID = ("y", "x", "zl")
ORDER = ("zh", "zl", "x", "y", "core")
MASK = 103

LATS = 8
PAIRS = 8
LANES = 128
HALF = 64
PITCH = 520
ROWS = 528
HELD = 3
DEPTH = 4
PARTS = 1
UNROLL = 2
VMEM = 60 * 2**20
STEP = 176


def exchange_places():
    ids = np.arange(np.prod(SIZES)).reshape(SIZES)
    order = ids.transpose([AXES.index(a) for a in ORDER]).reshape(-1)
    place = np.empty_like(order)
    place[order] = np.arange(order.size) ^ MASK
    return place


PLACE = exchange_places()


def pack_kernel(part, slots_in, weights_in, fourier, out, slots, weights, rows, blocks, sems, sent, small):
    waves = fourier.shape[1]
    pairs = blocks.shape[1]
    tables = (
        pltpu.make_async_copy(slots_in, slots, small.at[0]),
        pltpu.make_async_copy(weights_in, weights, small.at[1]),
    )
    for copy in tables:
        copy.start()

    def fetch(half, lat):
        return pltpu.make_async_copy(
            fourier.at[lat, :, pl.ds(half * LANES, LANES)],
            rows.at[half, pl.ds(lat * PITCH, waves), :],
            sems.at[half, lat],
        )

    for half in range(2):
        for lat in range(LATS):
            fetch(half, lat).start()
    for copy in tables:
        copy.wait()
    lat_ids = lax.broadcasted_iota(jnp.int32, (LATS, LANES), 0)
    scale = jnp.zeros((LATS, LANES), jnp.float32)
    for lat in range(LATS):
        scale = jnp.where(lat_ids == lat, weights[lat], scale)
    low = lax.broadcasted_iota(jnp.int32, (LATS, LANES), 1) < HALF
    for half in range(2):
        for lat in range(LATS):
            fetch(half, lat).wait()

        @pl.loop(0, 8 // UNROLL)
        def _(turn):
            for u in range(UNROLL):
                step = turn * UNROLL + u
                zl, x = step >> 2, step & 3
                for y in range(4):
                    place = ((half * 8 + step) ^ (MASK >> 3)) * 8 + (y ^ (MASK >> 1 & 3)) * 2
                    for q in range(pairs):
                        first = slots[(x * 2 + zl) * PAIRS + (y * 8 * PAIRS + part * pairs + q)]
                        second = waves - 1 - first
                        a = rows[half, pl.ds(first, LATS, stride=PITCH), :] * scale
                        b = rows[half, pl.ds(second, LATS, stride=PITCH), :] * scale
                        turned = pltpu.roll(b, HALF, 1)
                        blocks[place + (MASK & 1), q] = jnp.where(low, a, turned)
                        blocks[place + (1 - (MASK & 1)), q] = jnp.where(low, turned, a)
            at = pl.ds(((half * (8 // UNROLL) + turn) ^ (MASK // (8 * UNROLL))) * (8 * UNROLL), UNROLL * 8)
            pltpu.make_async_copy(blocks.at[at], out.at[at], sent).start()

    pltpu.make_async_copy(blocks, out, sent).wait()


def pack(part, pair_slots, weights, fourier):
    shape = (int(np.prod(SIZES)), PAIRS // PARTS, LATS, LANES)
    return pl.pallas_call(
        functools.partial(pack_kernel, part),
        name="pack",
        out_shape=jax.ShapeDtypeStruct(shape, jnp.float32),
        in_specs=[pl.BlockSpec(memory_space=pl.ANY)] * 3,
        out_specs=pl.BlockSpec(memory_space=pl.ANY),
        scratch_shapes=[
            pltpu.SMEM(pair_slots.shape, jnp.int32),
            pltpu.SMEM(weights.shape, jnp.float32),
            pltpu.VMEM((2, LATS * PITCH, LANES), jnp.float32),
            pltpu.VMEM(shape, jnp.float32),
            pltpu.SemaphoreType.DMA((2, LATS)),
            pltpu.SemaphoreType.DMA,
            pltpu.SemaphoreType.DMA((2,)),
        ],
        compiler_params=pltpu.CompilerParams(vmem_limit_bytes=VMEM),
        cost_estimate=pl.CostEstimate(flops=4 * 2**20, bytes_accessed=8 * 2**20, transcendentals=0),
    )(pair_slots, weights, fourier)


def split_kernel(legendre, high, low):
    rows = legendre.shape[0] // PAIRS
    for q in range(PAIRS):
        part = legendre[pl.ds(q, rows, stride=PAIRS), :]
        top = part.astype(jnp.bfloat16)
        high[q] = top
        low[q] = (part - top.astype(jnp.float32)).astype(jnp.bfloat16)


def split(legendre):
    lats = legendre.shape[1]
    shape = jax.ShapeDtypeStruct((PAIRS, ROWS, lats), jnp.bfloat16)
    spec = pl.BlockSpec((PAIRS, STEP, LANES), lambda i, j: (0, i, j))
    return pl.pallas_call(
        split_kernel,
        name="split",
        grid=(ROWS // STEP, lats // LANES),
        out_shape=(shape, shape),
        in_specs=[pl.BlockSpec((STEP * PAIRS, LANES), lambda i, j: (i, j))],
        out_specs=(spec, spec),
        compiler_params=pltpu.CompilerParams(vmem_limit_bytes=VMEM),
        cost_estimate=pl.CostEstimate(flops=2 * 10**10, bytes_accessed=32 * 2**20, transcendentals=0),
    )(legendre)


def hold_kernel(high, low, *rest):
    outs, sems = rest[:-1], rest[-1]
    copies = []
    for i, out in enumerate(outs):
        source = (high, low)[i % 2].at[i // 2]
        copies.append(pltpu.make_async_copy(source, out, sems.at[i]))
    for copy in copies:
        copy.start()
    for copy in copies:
        copy.wait()


def hold(high, low):
    shape = pltpu.VMEM(high.shape[1:], high.dtype)
    return pl.pallas_call(
        hold_kernel,
        name="hold",
        out_shape=[shape] * HELD,
        in_specs=[pl.BlockSpec(memory_space=pl.ANY)] * 2,
        out_specs=[pl.BlockSpec(memory_space=pltpu.VMEM)] * HELD,
        scratch_shapes=[pltpu.SemaphoreType.DMA((HELD,))],
        compiler_params=pltpu.CompilerParams(vmem_limit_bytes=20 * 2**20),
        cost_estimate=pl.CostEstimate(flops=2 * 10**9, bytes_accessed=4 * 2**20, transcendentals=0),
    )(high, low)


def sum_kernel(part, slots_in, where_in, high, low, values, *rest):
    held, out, scratch = rest[:HELD], rest[HELD], rest[HELD + 1 :]
    slots, where, highs, lows, inputs, results, terms, sums, sems, sent, small = scratch
    pairs, _, degrees = results.shape
    tables = (
        pltpu.make_async_copy(slots_in, slots, small.at[0]),
        pltpu.make_async_copy(where_in, where, small.at[1]),
    )

    def fetch_values(q):
        return pltpu.make_async_copy(values.at[:, q], inputs.at[q], sems.at[0, q])

    def fetch_matrix(q):
        terms_of = ((high, highs), (low, lows))
        return [
            pltpu.make_async_copy(source.at[part * pairs + q], target.at[q % DEPTH], sems.at[1 + i, q])
            for i, (source, target) in enumerate(terms_of)
            if 2 * q + i >= HELD
        ]

    def matrix(q, low_term):
        at = 2 * q + low_term
        return held[at][...] if at < HELD else (highs, lows)[low_term][q % DEPTH]

    def start(q):
        if q < pairs:
            for copy in fetch_matrix(q):
                copy.start()
        if q + 1 < pairs:
            fetch_values(q + 1).start()

    def prepare(q):
        for d, place in enumerate(PLACE):
            value = inputs[q, int(place)]
            top = value.astype(jnp.bfloat16)
            at = pl.ds(d * LATS, LATS)
            terms[q % 2, at, :LANES] = top
            terms[q % 2, at, LANES:] = (value - top.astype(jnp.float32)).astype(jnp.bfloat16)

    def multiply(q):
        dot = functools.partial(jnp.dot, preferred_element_type=jnp.float32)
        wide = dot(matrix(q, 0), terms[q % 2])
        sums[q % 2] = wide[:, :LANES] + wide[:, LANES:] + dot(matrix(q, 1), terms[q % 2, :, :LANES])

    def finish(q):
        turned = sums[q % 2].T[:, :degrees]
        limit = degrees - 1 - slots[where[0] * PAIRS + part * pairs + q]
        in_first = lax.broadcasted_iota(jnp.int32, (HALF, degrees), 1) < limit
        in_low = jnp.logical_xor(in_first, where[1] == 1)
        results[q] = jnp.where(in_low, turned[:HALF], turned[HALF:])

    def send(q):
        pltpu.make_async_copy(results.at[q], out.at[q], sent).start()

    fetch_values(0).start()
    for q in range(DEPTH - 1):
        start(q)
    for copy in tables:
        copy.start()
    fetch_values(0).wait()
    prepare(0)
    for q in range(pairs):
        start(q + DEPTH - 1)
        for copy in fetch_matrix(q):
            copy.wait()
        if q + 1 < pairs:
            fetch_values(q + 1).wait()
            prepare(q + 1)
        if q == 1:
            for copy in tables:
                copy.wait()
        multiply(q)
        if q:
            finish(q - 1)
            send(q - 1)
    finish(pairs - 1)
    send(pairs - 1)
    pltpu.make_async_copy(results, out, sent).wait()


def sums(part, pair_slots, where, high, low, values, held, degrees):
    lats = high.shape[2]
    devices, pairs = values.shape[:2]
    any_space = pl.BlockSpec(memory_space=pl.ANY)
    return pl.pallas_call(
        functools.partial(sum_kernel, part),
        name="sums",
        out_shape=jax.ShapeDtypeStruct((pairs, HALF, degrees), jnp.float32),
        in_specs=[any_space] * 5 + [pl.BlockSpec(memory_space=pltpu.VMEM)] * HELD,
        out_specs=any_space,
        scratch_shapes=[
            pltpu.SMEM(pair_slots.shape, jnp.int32),
            pltpu.SMEM(where.shape, jnp.int32),
            pltpu.VMEM((DEPTH, ROWS, lats), jnp.bfloat16),
            pltpu.VMEM((DEPTH, ROWS, lats), jnp.bfloat16),
            pltpu.VMEM((pairs, devices, LATS, LANES), jnp.float32),
            pltpu.VMEM((pairs, HALF, degrees), jnp.float32),
            pltpu.VMEM((2, lats, 2 * LANES), jnp.bfloat16),
            pltpu.VMEM((2, ROWS, LANES), jnp.float32),
            pltpu.SemaphoreType.DMA((3, pairs)),
            pltpu.SemaphoreType.DMA,
            pltpu.SemaphoreType.DMA((2,)),
        ],
        compiler_params=pltpu.CompilerParams(
            vmem_limit_bytes=40 * 2**20,
        ),
        cost_estimate=pl.CostEstimate(flops=6 * 2**30 // PARTS, bytes_accessed=24 * 2**20 // PARTS, transcendentals=0),
    )(pair_slots, where, high, low, values, *held)


def shards(fourier, weights, legendre, pair_slots):
    degrees, lats = legendre.shape[1:]
    owned = []
    for part in range(PARTS):
        packed = pack(part, pair_slots, weights, fourier)
        group = [int(device) for device in np.argsort(PLACE)]
        owned.append(
            lax.all_to_all(packed, AXES, split_axis=0, concat_axis=0, axis_index_groups=[group], tiled=True)
        )
    high, low = split(jnp.transpose(legendre, (1, 0, 2)).reshape(degrees * PAIRS, lats))
    held = hold(high, low)
    where = jnp.stack([lax.axis_index(GRID), lax.axis_index("core")]).astype(jnp.int32)
    results = [sums(part, pair_slots, where, high, low, owned[part], held, degrees) for part in range(PARTS)]
    result = results[0] if PARTS == 1 else jnp.concatenate(results, axis=0)
    return jnp.transpose(result, (0, 2, 1))


def solution(mesh):
    parts = Mesh(mesh.devices.reshape(SIZES), AXES)
    in_specs = (P(AXES, None, None), P(AXES), P(GRID, None, None), P())
    out_specs = P(GRID, None, LAYER)
    return jax.shard_map(shards, mesh=parts, in_specs=in_specs, out_specs=out_specs, check_vma=False)
```

```python
import functools

import jax
import jax.numpy as jnp
import numpy as np
from jax import lax
from jax.experimental import pallas as pl
from jax.experimental.pallas import tpu as pltpu
from jax.sharding import Mesh, PartitionSpec as P

AXES = ("zh", "core", "y", "x", "zl")
SIZES = (2, 2, 4, 4, 2)
LAYER = ("zh", "core")
GRID = ("y", "x", "zl")
ORDER = ("zh", "zl", "x", "y", "core")
MASK = 63

LATS = 8
PAIRS = 8
LANES = 128
HALF = 64
PITCH = 520
ROWS = 528
HELD = 3
DEPTH = 4
PARTS = 1
UNROLL = 2
VMEM = 60 * 2**20
STEP = 176


def exchange_places():
    ids = np.arange(np.prod(SIZES)).reshape(SIZES)
    order = ids.transpose([AXES.index(a) for a in ORDER]).reshape(-1)
    place = np.empty_like(order)
    place[order] = np.arange(order.size) ^ MASK
    return place


PLACE = exchange_places()


def pack_kernel(part, slots_in, weights_in, fourier, out, slots, weights, rows, blocks, sems, sent, small):
    waves = fourier.shape[1]
    pairs = blocks.shape[1]
    tables = (
        pltpu.make_async_copy(slots_in, slots, small.at[0]),
        pltpu.make_async_copy(weights_in, weights, small.at[1]),
    )
    for copy in tables:
        copy.start()

    def fetch(half, lat):
        return pltpu.make_async_copy(
            fourier.at[lat, :, pl.ds(half * LANES, LANES)],
            rows.at[half, pl.ds(lat * PITCH, waves), :],
            sems.at[half, lat],
        )

    for half in range(2):
        for lat in range(LATS):
            fetch(half, lat).start()
    for copy in tables:
        copy.wait()
    lat_ids = lax.broadcasted_iota(jnp.int32, (LATS, LANES), 0)
    scale = jnp.zeros((LATS, LANES), jnp.float32)
    for lat in range(LATS):
        scale = jnp.where(lat_ids == lat, weights[lat], scale)
    low = lax.broadcasted_iota(jnp.int32, (LATS, LANES), 1) < HALF
    for half in range(2):
        for lat in range(LATS):
            fetch(half, lat).wait()

        @pl.loop(0, 8 // UNROLL)
        def _(turn):
            for u in range(UNROLL):
                step = turn * UNROLL + u
                zl, x = step >> 2, step & 3
                for y in range(4):
                    place = ((half * 8 + step) ^ (MASK >> 3)) * 8 + (y ^ (MASK >> 1 & 3)) * 2
                    for q in range(pairs):
                        first = slots[(x * 2 + zl) * PAIRS + (y * 8 * PAIRS + part * pairs + q)]
                        second = waves - 1 - first
                        a = rows[half, pl.ds(first, LATS, stride=PITCH), :] * scale
                        b = rows[half, pl.ds(second, LATS, stride=PITCH), :] * scale
                        turned = pltpu.roll(b, HALF, 1)
                        blocks[place + (MASK & 1), q] = jnp.where(low, a, turned)
                        blocks[place + (1 - (MASK & 1)), q] = jnp.where(low, turned, a)
            at = pl.ds(((half * (8 // UNROLL) + turn) ^ (MASK // (8 * UNROLL))) * (8 * UNROLL), UNROLL * 8)
            pltpu.make_async_copy(blocks.at[at], out.at[at], sent).start()

    pltpu.make_async_copy(blocks, out, sent).wait()


def pack(part, pair_slots, weights, fourier):
    shape = (int(np.prod(SIZES)), PAIRS // PARTS, LATS, LANES)
    return pl.pallas_call(
        functools.partial(pack_kernel, part),
        name="pack",
        out_shape=jax.ShapeDtypeStruct(shape, jnp.float32),
        in_specs=[pl.BlockSpec(memory_space=pl.ANY)] * 3,
        out_specs=pl.BlockSpec(memory_space=pl.ANY),
        scratch_shapes=[
            pltpu.SMEM(pair_slots.shape, jnp.int32),
            pltpu.SMEM(weights.shape, jnp.float32),
            pltpu.VMEM((2, LATS * PITCH, LANES), jnp.float32),
            pltpu.VMEM(shape, jnp.float32),
            pltpu.SemaphoreType.DMA((2, LATS)),
            pltpu.SemaphoreType.DMA,
            pltpu.SemaphoreType.DMA((2,)),
        ],
        compiler_params=pltpu.CompilerParams(vmem_limit_bytes=VMEM),
        cost_estimate=pl.CostEstimate(flops=4 * 2**20, bytes_accessed=8 * 2**20, transcendentals=0),
    )(pair_slots, weights, fourier)


def split_kernel(legendre, high, low):
    rows = legendre.shape[0] // PAIRS
    for q in range(PAIRS):
        part = legendre[pl.ds(q, rows, stride=PAIRS), :]
        top = part.astype(jnp.bfloat16)
        high[q] = top
        low[q] = (part - top.astype(jnp.float32)).astype(jnp.bfloat16)


def split(legendre):
    lats = legendre.shape[1]
    shape = jax.ShapeDtypeStruct((PAIRS, ROWS, lats), jnp.bfloat16)
    spec = pl.BlockSpec((PAIRS, STEP, LANES), lambda i, j: (0, i, j))
    return pl.pallas_call(
        split_kernel,
        name="split",
        grid=(ROWS // STEP, lats // LANES),
        out_shape=(shape, shape),
        in_specs=[pl.BlockSpec((STEP * PAIRS, LANES), lambda i, j: (i, j))],
        out_specs=(spec, spec),
        compiler_params=pltpu.CompilerParams(vmem_limit_bytes=VMEM),
        cost_estimate=pl.CostEstimate(flops=2 * 10**10, bytes_accessed=32 * 2**20, transcendentals=0),
    )(legendre)


def hold_kernel(high, low, *rest):
    outs, sems = rest[:-1], rest[-1]
    copies = []
    for i, out in enumerate(outs):
        source = (high, low)[i % 2].at[i // 2]
        copies.append(pltpu.make_async_copy(source, out, sems.at[i]))
    for copy in copies:
        copy.start()
    for copy in copies:
        copy.wait()


def hold(high, low):
    shape = pltpu.VMEM(high.shape[1:], high.dtype)
    return pl.pallas_call(
        hold_kernel,
        name="hold",
        out_shape=[shape] * HELD,
        in_specs=[pl.BlockSpec(memory_space=pl.ANY)] * 2,
        out_specs=[pl.BlockSpec(memory_space=pltpu.VMEM)] * HELD,
        scratch_shapes=[pltpu.SemaphoreType.DMA((HELD,))],
        compiler_params=pltpu.CompilerParams(vmem_limit_bytes=20 * 2**20),
        cost_estimate=pl.CostEstimate(flops=2 * 10**9, bytes_accessed=4 * 2**20, transcendentals=0),
    )(high, low)


def sum_kernel(part, slots_in, where_in, high, low, values, *rest):
    held, out, scratch = rest[:HELD], rest[HELD], rest[HELD + 1 :]
    slots, where, highs, lows, inputs, results, terms, sums, sems, sent, small = scratch
    pairs, _, degrees = results.shape
    tables = (
        pltpu.make_async_copy(slots_in, slots, small.at[0]),
        pltpu.make_async_copy(where_in, where, small.at[1]),
    )

    def fetch_values(q):
        return pltpu.make_async_copy(values.at[:, q], inputs.at[q], sems.at[0, q])

    def fetch_matrix(q):
        terms_of = ((high, highs), (low, lows))
        return [
            pltpu.make_async_copy(source.at[part * pairs + q], target.at[q % DEPTH], sems.at[1 + i, q])
            for i, (source, target) in enumerate(terms_of)
            if 2 * q + i >= HELD
        ]

    def matrix(q, low_term):
        at = 2 * q + low_term
        return held[at][...] if at < HELD else (highs, lows)[low_term][q % DEPTH]

    def start(q):
        if q < pairs:
            for copy in fetch_matrix(q):
                copy.start()
        if q + 1 < pairs:
            fetch_values(q + 1).start()

    def prepare(q):
        for d, place in enumerate(PLACE):
            value = inputs[q, int(place)]
            top = value.astype(jnp.bfloat16)
            at = pl.ds(d * LATS, LATS)
            terms[q % 2, at, :LANES] = top
            terms[q % 2, at, LANES:] = (value - top.astype(jnp.float32)).astype(jnp.bfloat16)

    def multiply(q):
        dot = functools.partial(jnp.dot, preferred_element_type=jnp.float32)
        wide = dot(matrix(q, 0), terms[q % 2])
        sums[q % 2] = wide[:, :LANES] + wide[:, LANES:] + dot(matrix(q, 1), terms[q % 2, :, :LANES])

    def finish(q):
        turned = sums[q % 2].T[:, :degrees]
        limit = degrees - 1 - slots[where[0] * PAIRS + part * pairs + q]
        in_first = lax.broadcasted_iota(jnp.int32, (HALF, degrees), 1) < limit
        in_low = jnp.logical_xor(in_first, where[1] == 1)
        results[q] = jnp.where(in_low, turned[:HALF], turned[HALF:])

    def send(q):
        pltpu.make_async_copy(results.at[q], out.at[q], sent).start()

    fetch_values(0).start()
    for q in range(DEPTH - 1):
        start(q)
    for copy in tables:
        copy.start()
    fetch_values(0).wait()
    prepare(0)
    for q in range(pairs):
        start(q + DEPTH - 1)
        for copy in fetch_matrix(q):
            copy.wait()
        if q + 1 < pairs:
            fetch_values(q + 1).wait()
            prepare(q + 1)
        if q == 1:
            for copy in tables:
                copy.wait()
        multiply(q)
        if q:
            finish(q - 1)
            send(q - 1)
    finish(pairs - 1)
    send(pairs - 1)
    pltpu.make_async_copy(results, out, sent).wait()


def sums(part, pair_slots, where, high, low, values, held, degrees):
    lats = high.shape[2]
    devices, pairs = values.shape[:2]
    any_space = pl.BlockSpec(memory_space=pl.ANY)
    return pl.pallas_call(
        functools.partial(sum_kernel, part),
        name="sums",
        out_shape=jax.ShapeDtypeStruct((pairs, HALF, degrees), jnp.float32),
        in_specs=[any_space] * 5 + [pl.BlockSpec(memory_space=pltpu.VMEM)] * HELD,
        out_specs=any_space,
        scratch_shapes=[
            pltpu.SMEM(pair_slots.shape, jnp.int32),
            pltpu.SMEM(where.shape, jnp.int32),
            pltpu.VMEM((DEPTH, ROWS, lats), jnp.bfloat16),
            pltpu.VMEM((DEPTH, ROWS, lats), jnp.bfloat16),
            pltpu.VMEM((pairs, devices, LATS, LANES), jnp.float32),
            pltpu.VMEM((pairs, HALF, degrees), jnp.float32),
            pltpu.VMEM((2, lats, 2 * LANES), jnp.bfloat16),
            pltpu.VMEM((2, ROWS, LANES), jnp.float32),
            pltpu.SemaphoreType.DMA((3, pairs)),
            pltpu.SemaphoreType.DMA,
            pltpu.SemaphoreType.DMA((2,)),
        ],
        compiler_params=pltpu.CompilerParams(
            vmem_limit_bytes=40 * 2**20,
        ),
        cost_estimate=pl.CostEstimate(flops=6 * 2**30 // PARTS, bytes_accessed=24 * 2**20 // PARTS, transcendentals=0),
    )(pair_slots, where, high, low, values, *held)


def shards(fourier, weights, legendre, pair_slots):
    degrees, lats = legendre.shape[1:]
    owned = []
    for part in range(PARTS):
        packed = pack(part, pair_slots, weights, fourier)
        group = [int(device) for device in np.argsort(PLACE)]
        owned.append(
            lax.all_to_all(packed, AXES, split_axis=0, concat_axis=0, axis_index_groups=[group], tiled=True)
        )
    high, low = split(jnp.transpose(legendre, (1, 0, 2)).reshape(degrees * PAIRS, lats))
    held = hold(high, low)
    where = jnp.stack([lax.axis_index(GRID), lax.axis_index("core")]).astype(jnp.int32)
    results = [sums(part, pair_slots, where, high, low, owned[part], held, degrees) for part in range(PARTS)]
    result = results[0] if PARTS == 1 else jnp.concatenate(results, axis=0)
    return jnp.transpose(result, (0, 2, 1))


def solution(mesh):
    parts = Mesh(mesh.devices.reshape(SIZES), AXES)
    in_specs = (P(AXES, None, None), P(AXES), P(GRID, None, None), P())
    out_specs = P(GRID, None, LAYER)
    return jax.shard_map(shards, mesh=parts, in_specs=in_specs, out_specs=out_specs, check_vma=False)
```
